32 devices in a mesh: dp: 16 (over z, x, core), mp: 2 (over y).
Axes of the slice: x: 2, y: 2, z: 4, core: 2. Of those that a mesh axis runs over, the one named last changes fastest.
Arguments:
- node_feats: bfloat16 [256, 32768], P('mp', 'dp'), may hold values from -6 to 6
- proj_weight: bfloat16 [256, 256], P('mp'), may hold values from -0.375 to 0.375
- att_src: float32 [256], P('mp'), may hold values from -32 to 32
- att_dst: float32 [256], P('mp'), may hold values from -32 to 32
- out_bias: float32 [256], P('mp'), may hold values from -3 to 3
- tile_rows: int32 [512], P('dp'), may hold values from 0 to 255, as said below
- tile_cols: int32 [512], P('dp'), may hold values from 0 to 255, as said below
- tile_masks: int32 [512, 4, 128], P('dp'), may hold values from -2147483648 to 2147483646
Outputs:
- node_out: bfloat16 [256, 32768], P('mp', 'dp')
The draws below stay inside these ranges and needn't reach their ends.
Inputs may be any that keep to these rules, and one draw needn't show every extreme that they name: `tile_rows`: block b holds nodes 128 b to 128 b + 127 and belongs to index b // 16 of dp. Among the 32 tiles of one index of dp, no owner's blocks are named more than 4 times; on every index one owner's blocks are named exactly 4 times. `tile_cols`: the same bound holds for source blocks: among the 32 tiles of one index of dp, no owner's blocks are named more than 4 times, and one owner's exactly 4 times on every index.
All inputs are finite; a program needn't handle non-finite values.
Results may differ from the reference program's by a relative error of at most 0.0034.
Values may be sent and summed in bfloat16 or wider, within the bound.
A program may use at most 64 MiB of HBM per device.

```python
import jax
import jax.numpy as jnp
from jax import lax

FIN = 256
HEADS = 8
HD = 32
TILE = 128
TILES_DEV = 32
NODES = 32768
BLK_DEV = 16
NBLK = 256
TILES = 512
CAP = 4
N_DP = 16


def tile_blocks(key, salt):
    base_key = jax.random.fold_in(key, salt)
    hub_owner = jax.random.randint(jax.random.fold_in(base_key, 7), (), 0, N_DP)

    def device_tiles(device):
        device_key = jax.random.fold_in(base_key, device)
        key_rest, key_shift, key_local, key_order = jax.random.split(device_key, 4)
        rest_slots = CAP + jax.random.permutation(key_rest, N_DP * CAP - CAP)[:TILES_DEV - CAP]
        position = jnp.concatenate([jnp.arange(CAP, dtype=jnp.int32), rest_slots.astype(jnp.int32)])
        shifts = jnp.concatenate([jnp.zeros((1,), jnp.int32), 1 + jax.random.permutation(key_shift, N_DP - 1).astype(jnp.int32)])
        owners = (hub_owner + shifts[position // CAP]) % N_DP
        local_block = jax.random.randint(key_local, (TILES_DEV,), 0, BLK_DEV)
        blocks = owners * BLK_DEV + local_block
        return blocks[jax.random.permutation(key_order, TILES_DEV)]
    return jax.vmap(device_tiles)(jnp.arange(N_DP)).reshape(-1).astype(jnp.int32)


def draw_tile_rows(key, part):
    return tile_blocks(key, 101)


def draw_tile_cols(key, part):
    return tile_blocks(key, 202)


def attention_vector(key):
    key_base = jax.random.fold_in(key, 0)
    vector = 0.25 * jnp.clip(jax.random.normal(key_base, (HEADS, HD), jnp.float32), -4.0, 4.0)
    return vector.reshape(-1)


def draw_att_src(key, part):
    return attention_vector(jax.random.fold_in(key, 11))


def draw_att_dst(key, part):
    return attention_vector(jax.random.fold_in(key, 23))


def plant(entries, key, smallest, top_value):
    index_at = [jax.random.randint(jax.random.fold_in(key, axis), (), 0, length) for axis, length in enumerate(entries.shape)]
    widest = entries.shape.index(max(entries.shape))
    neighbour = index_at[:widest] + [(index_at[widest] + 1) % entries.shape[widest]] + index_at[widest + 1:]
    return entries.at[tuple(index_at)].set(smallest).at[tuple(neighbour)].set(top_value)


def levels(rng, shape, pieces, low, top_value):
    loudness, own = 1.0, jax.random.fold_in(rng, 6)
    for dim, parts in pieces:
        draws = jnp.exp(jax.random.uniform(jax.random.fold_in(own, dim), (parts,), jnp.float32, low / len(pieces), top_value / len(pieces)))
        loudness = loudness * jnp.repeat(draws, shape[dim] // parts).reshape([-1 if axis == dim else 1 for axis in range(len(shape))])
    return loudness


def bell_draw(stream_key, extent, width, limit, shards=(), held_as=jnp.bfloat16):
    values = width * jax.random.normal(stream_key, extent, jnp.float32)
    if shards:
        values = values * levels(stream_key, extent, shards, -0.22, 0.18)
    return jnp.clip(values, -limit, limit).astype(held_as)


def setup_inputs(seed: int = 0) -> dict:
    streams_of = jax.random.split(jax.random.key(seed), 9)
    return {
        "node_feats": bell_draw(streams_of[0], (FIN, NODES), 1.0, 6.0, ((0, 2), (1, 16))),
        "proj_weight": bell_draw(streams_of[1], (HEADS * HD, FIN), FIN ** -0.5, 0.375, ((0, 2),)),
        "att_src": draw_att_src(jax.random.fold_in(streams_of[8], 71), 0),
        "att_dst": draw_att_dst(jax.random.fold_in(streams_of[8], 71), 0),
        "out_bias": bell_draw(streams_of[4], (HEADS * HD,), 0.5, 3.0, ((0, 2),), jnp.float32),
        "tile_rows": draw_tile_rows(jax.random.fold_in(streams_of[8], 71), 0),
        "tile_cols": draw_tile_cols(jax.random.fold_in(streams_of[8], 71), 0),
        "tile_masks": plant(jax.random.randint(streams_of[7], (TILES, TILE // 32, TILE), -2147483648, 2147483647), jax.random.fold_in(streams_of[7], 1), -2147483648, 2147483646).astype(jnp.int32),
    }


far_below = -1.0e30


def leaky_relu(scores):
    return jnp.where(scores > 0, scores, 0.2 * scores)


def unpack_bits(packed):
    offsets = jnp.arange(32, dtype=jnp.int32)
    spread = jnp.bitwise_and(jnp.right_shift(packed[..., :, None, :], offsets[:, None]), 1)
    return spread.reshape(packed.shape[:-2] + (packed.shape[-2] * 32, packed.shape[-1])).astype(jnp.int32)


def edge_scores(edge_mask, source, target):
    raw_scores = leaky_relu(target[:, :, None, :] + source[:, :, :, None])
    return jnp.where(edge_mask[:, None] == 1, raw_scores, far_below)


def reference(node_feats, proj_weight, att_src, att_dst, out_bias, tile_rows, tile_cols, tile_masks):
    projected = jnp.dot(proj_weight, node_feats, preferred_element_type=jnp.float32)
    features = projected.astype(jnp.bfloat16)
    by_head = projected.reshape(HEADS, HD, NODES)
    source = jnp.einsum("hd,hdn->hn", att_src.reshape(HEADS, HD), by_head, precision=lax.Precision.HIGHEST)
    target = jnp.einsum("hd,hdn->hn", att_dst.reshape(HEADS, HD), by_head, precision=lax.Precision.HIGHEST)
    source_blocks = source.reshape(HEADS, NBLK, TILE).transpose(1, 0, 2)
    target_blocks = target.reshape(HEADS, NBLK, TILE).transpose(1, 0, 2)
    feat_blocks = features.reshape(HEADS, HD, NBLK, TILE).transpose(2, 0, 1, 3)
    group_rows = tile_rows.reshape(-1, TILES_DEV)
    group_cols = tile_cols.reshape(-1, TILES_DEV)
    group_masks = tile_masks.reshape(-1, TILES_DEV, TILE // 32, TILE)

    def tile_scores(inputs):
        row_ids, col_ids, packed = inputs
        edge_mask = unpack_bits(packed)
        scores = edge_scores(edge_mask, source_blocks[col_ids], target_blocks[row_ids])
        tile_peaks = jnp.max(scores, axis=2)
        weights = jnp.where(edge_mask[:, None] == 1, jnp.exp(scores - tile_peaks[:, :, None, :]), 0.0)
        return tile_peaks, weights

    def first_pass(inputs):
        tile_peaks, weights = tile_scores(inputs)
        return tile_peaks, jnp.sum(weights, axis=2)

    tile_peaks, masses = lax.map(first_pass, (group_rows, group_cols, group_masks))
    tile_peaks = tile_peaks.reshape(TILES, HEADS, TILE)
    masses = masses.reshape(TILES, HEADS, TILE)
    self_scores = leaky_relu(source_blocks + target_blocks)
    row_peak = self_scores.at[tile_rows].max(tile_peaks)
    self_weight = jnp.exp(self_scores - row_peak)
    denominator = self_weight.at[tile_rows].add(jnp.exp(tile_peaks - row_peak[tile_rows]) * masses)

    def second_pass(summed, inputs):
        row_ids, col_ids, packed = inputs
        peaks_here, weights = tile_scores(inputs)
        rounded = lax.optimization_barrier(weights.astype(jnp.bfloat16)).astype(jnp.float32)
        partial_values = jnp.einsum("ghdc,ghcr->ghdr", feat_blocks[col_ids].astype(jnp.float32), rounded)
        rescale = jnp.exp(peaks_here - row_peak[row_ids])
        return summed.at[row_ids].add(rescale[:, :, None, :] * partial_values), None

    start_sum = self_weight[:, :, None, :] * feat_blocks.astype(jnp.float32)
    summed, ignored = lax.scan(second_pass, start_sum, (group_rows, group_cols, group_masks))
    gathered = summed / denominator[:, :, None, :]
    flat_out = gathered.transpose(1, 2, 0, 3).reshape(HEADS * HD, NODES)
    return jax.nn.elu(flat_out + node_feats.astype(jnp.float32) + out_bias[:, None]).astype(jnp.bfloat16)
```

```python
import functools

import jax
import jax.numpy as jnp
from jax import lax
from jax.experimental import pallas as pl
from jax.experimental.pallas import tpu as pltpu
from jax.sharding import PartitionSpec as P

HD = 32
LOG2E = 1.4426950408889634
FAR_BELOW = -1e30
VMEM = pltpu.VMEM


def leaky_relu(scores):
    return jnp.maximum(scores, 0.2 * scores)


def project_kernel(heads, weight_ref, nodes_ref, att_src_ref, att_dst_ref, feats_ref, source_ref, target_ref):
    columns = nodes_ref.shape[1]
    step = 512 if columns % 512 == 0 else 128
    source_ref[...] = jnp.zeros_like(source_ref)
    target_ref[...] = jnp.zeros_like(target_ref)
    for start in range(0, columns, step):
        span = pl.ds(start, step)
        projected = jnp.dot(weight_ref[...], nodes_ref[:, span], preferred_element_type=jnp.float32)
        feats_ref[:, span] = projected.astype(jnp.bfloat16)
        to_source = projected * att_src_ref[...]
        to_target = projected * att_dst_ref[...]
        for head in range(heads):
            rows = slice(head * HD, (head + 1) * HD)
            source_ref[head : head + 1, span] = LOG2E * jnp.sum(to_source[rows], axis=0, keepdims=True)
            target_ref[head : head + 1, span] = LOG2E * jnp.sum(to_target[rows], axis=0, keepdims=True)


def tile_kernel(
    heads,
    code_ref,
    mask_ref,
    all_feats_ref,
    all_source_ref,
    feats_ref,
    source_ref,
    target_ref,
    nodes_ref,
    bias_ref,
    out_ref,
    total,
    best,
    mass,
):
    size = mask_ref.shape[2]
    blocks = nodes_ref.shape[1] // size
    all_blocks = blocks * all_feats_ref.shape[0]
    for block in range(blocks):
        span = slice(block * size, (block + 1) * size)
        best[block] = leaky_relu(source_ref[:, span] + target_ref[:, span])
        mass[block] = jnp.ones(mass.shape[1:], jnp.float32)
        total[block] = feats_ref[:, span].astype(jnp.float32)

    bit = lax.broadcasted_iota(jnp.int32, (32, size), 0)

    def tile(slot, carry):
        code = code_ref[slot]

        @pl.when(code >= 0)
        def _():
            row = lax.div(code, all_blocks)
            column = lax.rem(code, all_blocks)
            owner = lax.div(column, blocks)
            across = pl.ds(pl.multiple_of(lax.rem(column, blocks) * size, size), size)
            down = pl.ds(pl.multiple_of(row * size, size), size)
            packed = mask_ref[slot]
            edges = jnp.concatenate(
                [
                    jnp.bitwise_and(jnp.right_shift(packed[word : word + 1, :], bit), 1)
                    for word in range(size // 32)
                ],
                axis=0,
            ) != 0
            source = jnp.transpose(all_source_ref[owner, :, across])
            target = target_ref[:, down]
            for head in range(heads):
                rows = slice(head * HD, (head + 1) * HD)
                one = slice(head, head + 1)
                here = jnp.where(edges, source[:, one], FAR_BELOW)
                aim = target[one]
                old = best[row, one]
                peak = leaky_relu(aim + jnp.max(here, axis=0, keepdims=True))
                new = jnp.maximum(old, peak)
                weights = jnp.exp2(leaky_relu(here + aim) - new)
                value = jnp.dot(
                    all_feats_ref[owner, rows, across],
                    weights.astype(jnp.bfloat16),
                    preferred_element_type=jnp.float32,
                )
                keep = jnp.exp2(old - new)
                best[row, one] = new
                mass[row, one] = mass[row, one] * keep + jnp.sum(weights, axis=0, keepdims=True)
                total[row, rows] = total[row, rows] * keep + value

        return carry

    lax.fori_loop(0, code_ref.shape[0], tile, 0)

    for block in range(blocks):
        span = slice(block * size, (block + 1) * size)
        for head in range(heads):
            rows = slice(head * HD, (head + 1) * HD)
            shared = 1.0 / mass[block, head : head + 1]
            flat = total[block, rows] * shared + nodes_ref[rows, span].astype(jnp.float32) + bias_ref[rows]
            out_ref[rows, span] = jnp.where(flat > 0, flat, jnp.exp(flat) - 1.0).astype(out_ref.dtype)


def to_owners(tile_rows, tile_cols, tile_masks, blocks, devices):
    count = tile_rows.shape[0]
    capacity = max(2, 2 * count // devices)
    owners = tile_rows // blocks
    position = jnp.arange(count, dtype=jnp.int32)
    earlier = (owners[:, None] == owners[None, :]) & (position[None, :] < position[:, None])
    slots = owners * capacity + jnp.sum(earlier, axis=1)
    hits = slots[None, :] == jnp.arange(devices * capacity, dtype=jnp.int32)[:, None]
    codes = (tile_rows % blocks) * (blocks * devices) + tile_cols
    codes = jnp.sum(jnp.where(hits, codes[None, :] + 1, 0), axis=1) - 1
    tile_of = jnp.sum(jnp.where(hits, position[None, :], 0), axis=1)
    masks = jnp.take(tile_masks, tile_of, axis=0)
    return codes, masks, capacity


def local(node_feats, proj_weight, att_src, att_dst, out_bias, tile_rows, tile_cols, tile_masks):
    columns = node_feats.shape[1]
    head_dims = proj_weight.shape[0]
    heads = head_dims // HD
    padded = -(-heads // 8) * 8
    size = tile_masks.shape[2]
    blocks = columns // size
    devices = lax.axis_size("dp")
    codes, masks, capacity = to_owners(tile_rows, tile_cols, tile_masks, blocks, devices)
    words = masks.shape[1]
    payload = jnp.concatenate(
        [masks, jnp.broadcast_to(codes[:, None, None], (codes.shape[0], 1, size))], axis=1
    ).reshape(devices, capacity, words + 1, size)
    payload = lax.all_to_all(payload, "dp", split_axis=0, concat_axis=0, tiled=True)
    payload = payload.reshape(devices * capacity, words + 1, size)
    nodes = lax.all_gather(node_feats, "mp", axis=0, tiled=True)
    whole = pl.BlockSpec(memory_space=VMEM)
    feats, source, target = pl.pallas_call(
        functools.partial(project_kernel, heads),
        out_shape=(
            jax.ShapeDtypeStruct((head_dims, columns), jnp.bfloat16),
            jax.ShapeDtypeStruct((padded, columns), jnp.float32),
            jax.ShapeDtypeStruct((padded, columns), jnp.float32),
        ),
        in_specs=[whole] * 4,
        out_specs=(whole,) * 3,
        name="project",
    )(proj_weight, nodes, att_src[:, None], att_dst[:, None])
    all_feats = lax.all_gather(feats, "dp", axis=0)
    all_source = lax.all_gather(source, "dp", axis=0)
    return pl.pallas_call(
        functools.partial(tile_kernel, heads),
        out_shape=jax.ShapeDtypeStruct((head_dims, columns), jnp.bfloat16),
        in_specs=[pl.BlockSpec(memory_space=pltpu.SMEM)] + [whole] * 8,
        out_specs=whole,
        scratch_shapes=[
            VMEM((blocks, head_dims, size), jnp.float32),
            VMEM((blocks, padded, size), jnp.float32),
            VMEM((blocks, padded, size), jnp.float32),
        ],
        compiler_params=pltpu.CompilerParams(vmem_limit_bytes=40 * 1024 * 1024),
        name="tiles",
    )(
        payload[:, words, 0],
        payload[:, :words],
        all_feats,
        all_source,
        feats,
        source,
        target,
        node_feats,
        out_bias[:, None],
    )


def solution(mesh):
    return jax.shard_map(
        local,
        mesh=mesh,
        in_specs=(
            P("mp", "dp"),
            P("mp", None),
            P("mp"),
            P("mp"),
            P("mp"),
            P("dp"),
            P("dp"),
            P("dp", None, None),
        ),
        out_specs=P("mp", "dp"),
        check_vma=False,
    )
```

```python
import functools
import math

import jax
import jax.numpy as jnp
from jax import lax
from jax.experimental import pallas as pl
from jax.experimental.pallas import tpu as pltpu
from jax.sharding import PartitionSpec as P

HD = 32
LOG2E = 1.4426950408889634
FAR_BELOW = -1e30
VMEM = pltpu.VMEM


def leaky_relu(scores):
    return jnp.maximum(scores, 0.2 * scores)


def first_kernel(
    heads,
    capacity,
    chunks,
    ways,
    peers,
    weight_ref,
    nodes_ref,
    params_ref,
    payload_ref,
    tile_feats_ref,
    tile_source_ref,
    masks_ref,
    codes_ref,
    feats_ref,
    source_ref,
    target_ref,
    all_feats,
    all_source,
    all_nodes,
    got,
    codes,
    send_sem,
    recv_sem,
    node_send,
    node_recv,
    mask_send,
    mask_recv,
    code_sem,
):
    depth, across = ways
    devices = 2 * across * depth
    me = lax.axis_index("dp")
    core = lax.rem(me, 2)
    beside = lax.rem(lax.div(me, 2), across)
    level = lax.div(me, 2 * across)
    mine = lax.axis_index("mp")
    dims, columns = nodes_ref.shape
    head_dims = weight_ref.shape[0]
    size = payload_ref.shape[2]
    blocks = columns // size
    per = blocks // chunks
    width = per * size
    items = chunks + 1
    MESH = pl.DeviceIdType.MESH

    barrier = pltpu.get_barrier_semaphore()
    for shift in range(1, devices):
        pl.semaphore_signal(barrier, 1, device_id={"dp": lax.rem(me + shift, devices)}, device_id_type=MESH)
    for shift in range(1, peers):
        pl.semaphore_signal(barrier, 1, device_id={"mp": lax.rem(mine + shift, peers)}, device_id_type=MESH)
    own_rows = pl.ds(pl.multiple_of(mine * dims, dims), dims)
    for chunk in range(chunks):
        all_nodes[chunk, own_rows, :] = nodes_ref[:, chunk * width : (chunk + 1) * width]
    got[me] = payload_ref[me]
    params = jnp.transpose(params_ref[...])[:head_dims]
    pl.semaphore_wait(barrier, devices - 1 + peers - 1)

    def node_copy(shift, chunk):
        return pltpu.make_async_remote_copy(
            src_ref=nodes_ref.at[:, pl.ds(chunk * width, width)],
            dst_ref=all_nodes.at[chunk, own_rows, :],
            send_sem=node_send.at[shift - 1, chunk],
            recv_sem=node_recv.at[shift - 1, chunk],
            device_id={"mp": lax.rem(mine + shift, peers)},
            device_id_type=MESH,
        )

    def mask_copy(shift):
        to = lax.rem(me + shift, devices)
        return pltpu.make_async_remote_copy(
            src_ref=payload_ref.at[to],
            dst_ref=got.at[me],
            send_sem=mask_send.at[shift - 1],
            recv_sem=mask_recv.at[shift - 1],
            device_id={"dp": to},
            device_id_type=MESH,
        )

    for chunk in range(chunks):
        for shift in range(1, peers):
            node_copy(shift, chunk).start()
    for shift in range(1, devices):
        mask_copy(shift).start()

    def place(a, b, c):
        return (a * across + b) * 2 + c

    down = place(jnp.maximum(level - 1, 0), beside, core)
    up = place(jnp.minimum(level + 1, depth - 1), beside, core)
    facing = place(level, across - 1 - beside, core)
    partner = place(level, beside, 1 - core)
    targets = (down, up, facing, partner)

    def copy(way, origin, item):
        if item < chunks:
            part = all_feats.at[pl.ds(origin * blocks + item * per, per)]
        else:
            part = all_source.at[pl.ds(origin * blocks, blocks)]
        return pltpu.make_async_remote_copy(
            src_ref=part,
            dst_ref=part,
            send_sem=send_sem.at[way, origin, item],
            recv_sem=recv_sem.at[origin, item],
            device_id={"dp": targets[way]},
            device_id_type=MESH,
        )

    def facing_first(item):
        return item == 0 and across > 1

    def project(chunk):
        for shift in range(1, peers):
            node_copy(shift, chunk).wait_recv()
        projected = jnp.dot(weight_ref[...], all_nodes[chunk], preferred_element_type=jnp.float32)
        rounded = projected.astype(jnp.bfloat16)
        for j in range(per):
            block = chunk * per + j
            span = slice(j * size, (j + 1) * size)
            all_feats[me * blocks + block] = rounded[:, span]
            feats_ref[block] = rounded[:, span]
        for j in range(per):
            block = chunk * per + j
            span = slice(j * size, (j + 1) * size)
            to_source = projected[:, span] * params[:, 0:1]
            to_target = projected[:, span] * params[:, 1:2]
            for head in range(heads):
                rows = slice(head * HD, (head + 1) * HD)
                one = slice(head, head + 1)
                score = LOG2E * jnp.sum(to_source[rows], axis=0, keepdims=True)
                source_ref[block, one] = score
                all_source[me * blocks + block, one] = score
                target_ref[block, one] = LOG2E * jnp.sum(to_target[rows], axis=0, keepdims=True)

    source_ref[...] = jnp.zeros_like(source_ref)
    target_ref[...] = jnp.zeros_like(target_ref)
    tile_source_ref[...] = jnp.zeros_like(tile_source_ref)

    def outward(origin, item):
        @pl.when(level > 0)
        def _():
            copy(0, origin, item).start()

        @pl.when(level < depth - 1)
        def _():
            copy(1, origin, item).start()

    def arrived(step, side, item):
        streams = [beside]
        if facing_first(item):
            streams.append(across - 1 - beside)

        @pl.when(level >= step if side == 1 else level + step < depth)
        def _():
            for stream in streams:
                origin = place(level - step if side == 1 else level + step, stream, core)
                copy(3, origin, item).wait_recv()

                @pl.when(level < depth - 1 if side == 1 else level > 0)
                def _():
                    copy(side, origin, item).start()

                if across > 1 and not facing_first(item):
                    copy(2, origin, item).start()
                copy(3, origin, item).start()

    def from_facing(step, side, item):
        @pl.when(level >= step if side == 1 else level + step < depth)
        def _():
            origin = place(level - step if side == 1 else level + step, across - 1 - beside, core)
            copy(3, origin, item).wait_recv()
            copy(3, origin, item).start()

    for time in range(items + depth):
        if time < items:
            if time < chunks:
                project(time)
            outward(me, time)
            if across > 1:
                copy(2, me, time).start()
            copy(3, me, time).start()
        if across > 1 and 0 <= time - 1 < items:
            origin = place(level, across - 1 - beside, core)
            copy(3, origin, time - 1).wait_recv()
            if facing_first(time - 1):
                outward(origin, time - 1)
            copy(3, origin, time - 1).start()
        for step in range(1, depth):
            item = time - step
            if 0 <= item < items:
                arrived(step, 1, item)
                arrived(step, 0, item)
            if across > 1 and 0 <= time - step - 1 < items and not facing_first(time - step - 1):
                from_facing(step, 1, time - step - 1)
                from_facing(step, 0, time - step - 1)

    for shift in range(1, devices):
        mask_copy(shift).wait()
    padded = codes.shape[1]
    rows = got.shape[1] - padded
    fetch = pltpu.make_async_copy(got.at[:, pl.ds(rows, padded), :], codes, code_sem)
    fetch.start()
    masks_ref[...] = got[:, :rows, :]
    codes_ref[...] = got[:, rows:, :]
    fetch.wait()
    for item in range(items):
        for a in range(depth):
            for b in range(across):
                copy(3, place(a, b, 1 - core), item).wait_recv()

    def pick(slot, carry):
        code = codes[lax.div(slot, capacity), 0, lax.rem(slot, capacity)]
        column = lax.rem(jnp.maximum(code, 0), blocks * devices)
        tile_feats_ref[slot] = all_feats[column]
        tile_source_ref[slot, :heads] = all_source[column]
        return carry

    lax.fori_loop(0, devices * capacity, pick, 0)

    for chunk in range(chunks):
        for shift in range(1, peers):
            node_copy(shift, chunk).wait_send()
    for item in range(items):
        for a in range(depth):
            for b in range(across):
                origin = place(a, b, core)
                copy(3, origin, item).wait_send()
                if facing_first(item):
                    to_facing = (a == level) & (b == beside)
                    moves = True
                else:
                    to_facing = b == beside
                    moves = b == beside
                if across > 1:

                    @pl.when(to_facing)
                    def _():
                        copy(2, origin, item).wait_send()

                @pl.when(moves & (level > 0) & (level <= a))
                def _():
                    copy(0, origin, item).wait_send()

                @pl.when(moves & (level < depth - 1) & (level >= a))
                def _():
                    copy(1, origin, item).wait_send()


def tile_kernel(
    heads,
    capacity,
    code_ref,
    mask_ref,
    tile_feats_ref,
    tile_source_ref,
    feats_ref,
    source_ref,
    target_ref,
    nodes_ref,
    params_ref,
    out_ref,
    total,
    best,
    mass,
):
    size = mask_ref.shape[2]
    blocks = nodes_ref.shape[1] // size
    all_blocks = blocks * mask_ref.shape[0]
    words = size // 32
    bias = jnp.transpose(params_ref[...])[:, 2:3]
    for block in range(blocks):
        best[block] = leaky_relu(source_ref[block] + target_ref[block])
        mass[block] = jnp.ones(mass.shape[1:], jnp.float32)
        total[block] = feats_ref[block].astype(jnp.float32)

    bit = lax.broadcasted_iota(jnp.int32, (32, size), 0)

    def tile(slot, carry):
        holder = lax.div(slot, capacity)
        turn = lax.rem(slot, capacity)
        code = code_ref[holder, 0, turn]

        @pl.when(code >= 0)
        def _():
            row = lax.div(code, all_blocks)
            packed = mask_ref[holder, pl.ds(turn * words, words), :]
            edges = jnp.concatenate(
                [
                    jnp.bitwise_and(jnp.right_shift(packed[word : word + 1, :], bit), 1)
                    for word in range(words)
                ],
                axis=0,
            ) != 0
            source = jnp.transpose(tile_source_ref[slot])
            target = target_ref[row]
            for head in range(heads):
                rows = slice(head * HD, (head + 1) * HD)
                one = slice(head, head + 1)
                here = jnp.where(edges, source[:, one], FAR_BELOW)
                aim = target[one]
                old = best[row, one]
                peak = leaky_relu(aim + jnp.max(here, axis=0, keepdims=True))
                new = jnp.maximum(old, peak)
                weights = jnp.exp2(leaky_relu(here + aim) - new)
                value = jnp.dot(
                    tile_feats_ref[slot, rows],
                    weights.astype(jnp.bfloat16),
                    preferred_element_type=jnp.float32,
                )
                keep = jnp.exp2(old - new)
                best[row, one] = new
                mass[row, one] = mass[row, one] * keep + jnp.sum(weights, axis=0, keepdims=True)
                total[row, rows] = total[row, rows] * keep + value

        return carry

    lax.fori_loop(0, mask_ref.shape[0] * capacity, tile, 0)

    for block in range(blocks):
        span = slice(block * size, (block + 1) * size)
        for head in range(heads):
            rows = slice(head * HD, (head + 1) * HD)
            shared = 1.0 / mass[block, head : head + 1]
            flat = total[block, rows] * shared + nodes_ref[rows, span].astype(jnp.float32) + bias[rows]
            out_ref[rows, span] = jnp.where(flat > 0, flat, jnp.exp(flat) - 1.0).astype(out_ref.dtype)


def to_owners(tile_rows, tile_cols, tile_masks, blocks, devices):
    count = tile_rows.shape[0]
    capacity = max(2, 2 * count // devices)
    owners = tile_rows // blocks
    position = jnp.arange(count, dtype=jnp.int32)
    earlier = (owners[:, None] == owners[None, :]) & (position[None, :] < position[:, None])
    slots = owners * capacity + jnp.sum(earlier, axis=1)
    hits = slots[None, :] == jnp.arange(devices * capacity, dtype=jnp.int32)[:, None]
    codes = (tile_rows % blocks) * (blocks * devices) + tile_cols
    codes = jnp.sum(jnp.where(hits, codes[None, :] + 1, 0), axis=1) - 1
    tile_of = jnp.sum(jnp.where(hits, position[None, :], 0), axis=1)
    masks = jnp.take(tile_masks, tile_of, axis=0)
    return codes, masks, capacity


def local(node_feats, proj_weight, att_src, att_dst, out_bias, tile_rows, tile_cols, tile_masks):
    columns = node_feats.shape[1]
    head_dims = proj_weight.shape[0]
    heads = head_dims // HD
    padded = -(-heads // 8) * 8
    size = tile_masks.shape[2]
    blocks = columns // size
    devices = lax.axis_size("dp")
    codes, masks, capacity = to_owners(tile_rows, tile_cols, tile_masks, blocks, devices)
    words = masks.shape[1]
    peers = lax.axis_size("mp")
    mask_rows = -(-capacity * words // 8) * 8
    payload = jnp.concatenate(
        [
            jnp.pad(
                masks.reshape(devices, capacity * words, size),
                ((0, 0), (0, mask_rows - capacity * words), (0, 0)),
            ),
            jnp.pad(codes.reshape(devices, 1, capacity), ((0, 0), (0, 7), (0, size - capacity))),
        ],
        axis=1,
    )
    params = jnp.pad(jnp.stack([att_src, att_dst, out_bias]), ((0, 5), (0, -head_dims % 128)))
    chips = devices // 2
    across = 2 if chips % 2 == 0 else 1
    ways = (chips // across, across)
    chunks = math.gcd(blocks, max(1, 128 // devices))
    items = chunks + 1
    slots = devices * capacity
    whole = pl.BlockSpec(memory_space=VMEM)
    dma = pltpu.SemaphoreType.DMA
    tile_feats, tile_source, masks, codes, feats, source, target = pl.pallas_call(
        functools.partial(first_kernel, heads, capacity, chunks, ways, peers),
        out_shape=(
            jax.ShapeDtypeStruct((slots, head_dims, size), jnp.bfloat16),
            jax.ShapeDtypeStruct((slots, padded, size), jnp.float32),
            jax.ShapeDtypeStruct((devices, mask_rows, size), jnp.int32),
            jax.ShapeDtypeStruct((devices, 8, size), jnp.int32),
            jax.ShapeDtypeStruct((blocks, head_dims, size), jnp.bfloat16),
            jax.ShapeDtypeStruct((blocks, padded, size), jnp.float32),
            jax.ShapeDtypeStruct((blocks, padded, size), jnp.float32),
        ),
        in_specs=[whole] * 4,
        out_specs=(whole,) * 7,
        scratch_shapes=[
            VMEM((devices * blocks, head_dims, size), jnp.bfloat16),
            VMEM((devices * blocks, heads, size), jnp.float32),
            VMEM((chunks, peers * node_feats.shape[0], columns // chunks), jnp.bfloat16),
            VMEM((devices, mask_rows + 8, size), jnp.int32),
            pltpu.SMEM((devices, 8, size), jnp.int32),
            dma((4, devices, items)),
            dma((devices, items)),
            dma((max(1, peers - 1), chunks)),
            dma((max(1, peers - 1), chunks)),
            dma((devices - 1,)),
            dma((devices - 1,)),
            dma,
        ],
        compiler_params=pltpu.CompilerParams(
            collective_id=0, has_side_effects=True, vmem_limit_bytes=40 * 1024 * 1024
        ),
        name="gather",
    )(proj_weight, node_feats, params, payload)
    return pl.pallas_call(
        functools.partial(tile_kernel, heads, capacity),
        out_shape=jax.ShapeDtypeStruct((head_dims, columns), jnp.bfloat16),
        in_specs=[pl.BlockSpec(memory_space=pltpu.SMEM)] + [whole] * 8,
        out_specs=whole,
        scratch_shapes=[
            VMEM((blocks, head_dims, size), jnp.float32),
            VMEM((blocks, padded, size), jnp.float32),
            VMEM((blocks, padded, size), jnp.float32),
        ],
        compiler_params=pltpu.CompilerParams(vmem_limit_bytes=40 * 1024 * 1024),
        name="tiles",
    )(codes, masks, tile_feats, tile_source, feats, source, target, node_feats, params)


def solution(mesh):
    return jax.shard_map(
        local,
        mesh=mesh,
        in_specs=(
            P("mp", "dp"),
            P("mp", None),
            P("mp"),
            P("mp"),
            P("mp"),
            P("dp"),
            P("dp"),
            P("dp", None, None),
        ),
        out_specs=P("mp", "dp"),
        check_vma=False,
    )
```

```python
import functools
import math

import jax
import jax.numpy as jnp
from jax import lax
from jax.experimental import pallas as pl
from jax.experimental.pallas import tpu as pltpu
from jax.sharding import PartitionSpec as P

HD = 32
LOG2E = 1.4426950408889634
FAR_BELOW = -1e30
VMEM = pltpu.VMEM


def leaky_relu(scores):
    return jnp.maximum(scores, 0.2 * scores)


def first_kernel(
    heads,
    capacity,
    chunks,
    ways,
    peers,
    weight_ref,
    nodes_ref,
    params_ref,
    payload_ref,
    tile_feats_ref,
    tile_source_ref,
    masks_ref,
    codes_ref,
    feats_ref,
    source_ref,
    target_ref,
    all_feats,
    all_source,
    all_nodes,
    got,
    codes,
    send_sem,
    recv_sem,
    node_send,
    node_recv,
    mask_send,
    mask_recv,
    code_sem,
):
    depth, across = ways
    devices = 2 * across * depth
    me = lax.axis_index("dp")
    core = lax.rem(me, 2)
    beside = lax.rem(lax.div(me, 2), across)
    level = lax.div(me, 2 * across)
    mine = lax.axis_index("mp")
    dims, columns = nodes_ref.shape
    head_dims = weight_ref.shape[0]
    size = payload_ref.shape[2]
    blocks = columns // size
    per = blocks // chunks
    width = per * size
    items = chunks + 1
    MESH = pl.DeviceIdType.MESH

    barrier = pltpu.get_barrier_semaphore()
    for shift in range(1, devices):
        pl.semaphore_signal(barrier, 1, device_id={"dp": lax.rem(me + shift, devices)}, device_id_type=MESH)
    for shift in range(1, peers):
        pl.semaphore_signal(barrier, 1, device_id={"mp": lax.rem(mine + shift, peers)}, device_id_type=MESH)
    own_rows = pl.ds(pl.multiple_of(mine * dims, dims), dims)
    for chunk in range(chunks):
        all_nodes[chunk, own_rows, :] = nodes_ref[:, chunk * width : (chunk + 1) * width]
    got[me] = payload_ref[me]
    params = jnp.transpose(params_ref[...])[:head_dims]
    pl.semaphore_wait(barrier, devices - 1 + peers - 1)

    def node_copy(shift, chunk):
        return pltpu.make_async_remote_copy(
            src_ref=nodes_ref.at[:, pl.ds(chunk * width, width)],
            dst_ref=all_nodes.at[chunk, own_rows, :],
            send_sem=node_send.at[shift - 1, chunk],
            recv_sem=node_recv.at[shift - 1, chunk],
            device_id={"mp": lax.rem(mine + shift, peers)},
            device_id_type=MESH,
        )

    def mask_copy(shift):
        to = lax.rem(me + shift, devices)
        return pltpu.make_async_remote_copy(
            src_ref=payload_ref.at[to],
            dst_ref=got.at[me],
            send_sem=mask_send.at[shift - 1],
            recv_sem=mask_recv.at[shift - 1],
            device_id={"dp": to},
            device_id_type=MESH,
        )

    for chunk in range(chunks):
        for shift in range(1, peers):
            node_copy(shift, chunk).start()
    for shift in range(1, devices):
        mask_copy(shift).start()

    def place(a, b, c):
        return (a * across + b) * 2 + c

    down = place(jnp.maximum(level - 1, 0), beside, core)
    up = place(jnp.minimum(level + 1, depth - 1), beside, core)
    facing = place(level, across - 1 - beside, core)
    partner = place(level, beside, 1 - core)
    targets = (down, up, facing, partner)

    def copy(way, origin, item):
        if item < chunks:
            part = all_feats.at[pl.ds(origin * blocks + item * per, per)]
        else:
            part = all_source.at[pl.ds(origin * blocks, blocks)]
        return pltpu.make_async_remote_copy(
            src_ref=part,
            dst_ref=part,
            send_sem=send_sem.at[way, origin, item],
            recv_sem=recv_sem.at[origin, item],
            device_id={"dp": targets[way]},
            device_id_type=MESH,
        )

    def facing_first(item):
        return item == 0 and across > 1

    def project(chunk):
        for shift in range(1, peers):
            node_copy(shift, chunk).wait_recv()
        projected = jnp.dot(weight_ref[...], all_nodes[chunk], preferred_element_type=jnp.float32)
        rounded = projected.astype(jnp.bfloat16)
        for j in range(per):
            block = chunk * per + j
            span = slice(j * size, (j + 1) * size)
            all_feats[me * blocks + block] = rounded[:, span]
            feats_ref[block] = rounded[:, span]
        for j in range(per):
            block = chunk * per + j
            span = slice(j * size, (j + 1) * size)
            to_source = projected[:, span] * params[:, 0:1]
            to_target = projected[:, span] * params[:, 1:2]
            for head in range(heads):
                rows = slice(head * HD, (head + 1) * HD)
                one = slice(head, head + 1)
                score = LOG2E * jnp.sum(to_source[rows], axis=0, keepdims=True)
                source_ref[block, one] = score
                all_source[me * blocks + block, one] = score
                target_ref[block, one] = LOG2E * jnp.sum(to_target[rows], axis=0, keepdims=True)

    source_ref[...] = jnp.zeros_like(source_ref)
    target_ref[...] = jnp.zeros_like(target_ref)
    tile_source_ref[...] = jnp.zeros_like(tile_source_ref)

    def outward(origin, item):
        @pl.when(level > 0)
        def _():
            copy(0, origin, item).start()

        @pl.when(level < depth - 1)
        def _():
            copy(1, origin, item).start()

    def arrived(step, side, item):
        streams = [beside]
        if facing_first(item):
            streams.append(across - 1 - beside)

        @pl.when(level >= step if side == 1 else level + step < depth)
        def _():
            for stream in streams:
                origin = place(level - step if side == 1 else level + step, stream, core)
                copy(3, origin, item).wait_recv()

                @pl.when(level < depth - 1 if side == 1 else level > 0)
                def _():
                    copy(side, origin, item).start()

                if across > 1 and not facing_first(item):
                    copy(2, origin, item).start()
                copy(3, origin, item).start()

    def from_facing(step, side, item):
        @pl.when(level >= step if side == 1 else level + step < depth)
        def _():
            origin = place(level - step if side == 1 else level + step, across - 1 - beside, core)
            copy(3, origin, item).wait_recv()
            copy(3, origin, item).start()

    def from_level(item):
        origin = place(level, across - 1 - beside, core)
        copy(3, origin, item).wait_recv()
        if facing_first(item):
            outward(origin, item)
        copy(3, origin, item).start()

    for item in range(items):
        if item < chunks:
            project(item)
        outward(me, item)
        if across > 1:
            copy(2, me, item).start()
        copy(3, me, item).start()
        if item == 2 and across > 1:
            from_level(0)
    for step in range(1, depth + 1):
        for item in range(items):
            if step < depth:
                arrived(step, 1, item)
                arrived(step, 0, item)
            if across > 1 and step == 1 and (item > 0 or items <= 2):
                from_level(item)
            if across > 1 and step > 1 and not facing_first(item):
                from_facing(step - 1, 1, item)
                from_facing(step - 1, 0, item)

    for shift in range(1, devices):
        mask_copy(shift).wait()
    padded = codes.shape[1]
    rows = got.shape[1] - padded
    fetch = pltpu.make_async_copy(got.at[:, pl.ds(rows, padded), :], codes, code_sem)
    fetch.start()
    masks_ref[...] = got[:, :rows, :]
    codes_ref[...] = got[:, rows:, :]
    fetch.wait()
    for item in range(items):
        for a in range(depth):
            for b in range(across):
                copy(3, place(a, b, 1 - core), item).wait_recv()

    def pick(slot, carry):
        code = codes[lax.div(slot, capacity), 0, lax.rem(slot, capacity)]
        column = lax.rem(jnp.maximum(code, 0), blocks * devices)
        tile_feats_ref[slot] = all_feats[column]
        tile_source_ref[slot, :heads] = all_source[column]
        return carry

    lax.fori_loop(0, devices * capacity, pick, 0)

    for chunk in range(chunks):
        for shift in range(1, peers):
            node_copy(shift, chunk).wait_send()
    for item in range(items):
        for a in range(depth):
            for b in range(across):
                origin = place(a, b, core)
                copy(3, origin, item).wait_send()
                if facing_first(item):
                    to_facing = (a == level) & (b == beside)
                    moves = True
                else:
                    to_facing = b == beside
                    moves = b == beside
                if across > 1:

                    @pl.when(to_facing)
                    def _():
                        copy(2, origin, item).wait_send()

                @pl.when(moves & (level > 0) & (level <= a))
                def _():
                    copy(0, origin, item).wait_send()

                @pl.when(moves & (level < depth - 1) & (level >= a))
                def _():
                    copy(1, origin, item).wait_send()


def tile_kernel(
    heads,
    capacity,
    code_ref,
    mask_ref,
    tile_feats_ref,
    tile_source_ref,
    feats_ref,
    source_ref,
    target_ref,
    nodes_ref,
    params_ref,
    out_ref,
    total,
    best,
    mass,
):
    size = mask_ref.shape[2]
    blocks = nodes_ref.shape[1] // size
    all_blocks = blocks * mask_ref.shape[0]
    words = size // 32
    bias = jnp.transpose(params_ref[...])[:, 2:3]
    for block in range(blocks):
        best[block] = leaky_relu(source_ref[block] + target_ref[block])
        mass[block] = jnp.ones(mass.shape[1:], jnp.float32)
        total[block] = feats_ref[block].astype(jnp.float32)

    bit = lax.broadcasted_iota(jnp.int32, (32, size), 0)

    def partial(slot):
        holder = lax.div(slot, capacity)
        turn = lax.rem(slot, capacity)
        row = lax.div(jnp.maximum(code_ref[holder, 0, turn], 0), all_blocks)
        packed = mask_ref[holder, pl.ds(turn * words, words), :]
        edges = jnp.concatenate(
            [
                jnp.bitwise_and(jnp.right_shift(packed[word : word + 1, :], bit), 1)
                for word in range(words)
            ],
            axis=0,
        ) != 0
        source = jnp.transpose(tile_source_ref[slot])
        target = target_ref[row]
        itself = leaky_relu(source_ref[row] + target)
        peaks, masses, values = [], [], []
        for head in range(heads):
            one = slice(head, head + 1)
            here = jnp.where(edges, source[:, one], FAR_BELOW)
            aim = target[one]
            peak = leaky_relu(aim + jnp.max(here, axis=0, keepdims=True))
            peak = jnp.maximum(itself[one], peak)
            weights = jnp.exp2(leaky_relu(here + aim) - peak)
            peaks.append(peak)
            masses.append(jnp.sum(weights, axis=0, keepdims=True))
            values.append(
                jnp.dot(
                    tile_feats_ref[slot, head * HD : (head + 1) * HD],
                    weights.astype(jnp.bfloat16),
                    preferred_element_type=jnp.float32,
                )
            )
        return row, peaks, masses, values

    def merge(row, peaks, masses, values):
        old = best[row, :heads]
        peak = jnp.concatenate(peaks, axis=0)
        new = jnp.maximum(old, peak)
        keep = jnp.exp2(old - new)
        scale = jnp.exp2(peak - new)
        best[row, :heads] = new
        mass[row, :heads] = mass[row, :heads] * keep + jnp.concatenate(masses, axis=0) * scale
        had = total[row]
        total[row] = jnp.concatenate(
            [
                had[head * HD : (head + 1) * HD] * keep[head : head + 1]
                + values[head] * scale[head : head + 1]
                for head in range(heads)
            ],
            axis=0,
        )

    slots = mask_ref.shape[0] * capacity
    together = math.gcd(slots, 2)

    def tiles(step, carry):
        parts = [partial(step * together + which) for which in range(together)]
        for part in parts:
            merge(*part)
        return carry

    lax.fori_loop(0, slots // together, tiles, 0)

    for block in range(blocks):
        span = slice(block * size, (block + 1) * size)
        for head in range(heads):
            rows = slice(head * HD, (head + 1) * HD)
            shared = 1.0 / mass[block, head : head + 1]
            flat = total[block, rows] * shared + nodes_ref[rows, span].astype(jnp.float32) + bias[rows]
            out_ref[rows, span] = jnp.where(flat > 0, flat, jnp.exp(flat) - 1.0).astype(out_ref.dtype)


def to_owners(tile_rows, tile_cols, tile_masks, blocks, devices):
    count = tile_rows.shape[0]
    capacity = max(2, 2 * count // devices)
    owners = tile_rows // blocks
    position = jnp.arange(count, dtype=jnp.int32)
    earlier = (owners[:, None] == owners[None, :]) & (position[None, :] < position[:, None])
    slots = owners * capacity + jnp.sum(earlier, axis=1)
    hits = slots[None, :] == jnp.arange(devices * capacity, dtype=jnp.int32)[:, None]
    codes = (tile_rows % blocks) * (blocks * devices) + tile_cols
    codes = jnp.sum(jnp.where(hits, codes[None, :] + 1, 0), axis=1) - 1
    tile_of = jnp.sum(jnp.where(hits, position[None, :], 0), axis=1)
    masks = jnp.where(codes[:, None, None] >= 0, jnp.take(tile_masks, tile_of, axis=0), 0)
    return codes, masks, capacity


def local(node_feats, proj_weight, att_src, att_dst, out_bias, tile_rows, tile_cols, tile_masks):
    columns = node_feats.shape[1]
    head_dims = proj_weight.shape[0]
    heads = head_dims // HD
    padded = -(-heads // 8) * 8
    size = tile_masks.shape[2]
    blocks = columns // size
    devices = lax.axis_size("dp")
    codes, masks, capacity = to_owners(tile_rows, tile_cols, tile_masks, blocks, devices)
    words = masks.shape[1]
    peers = lax.axis_size("mp")
    mask_rows = -(-capacity * words // 8) * 8
    payload = jnp.concatenate(
        [
            jnp.pad(
                masks.reshape(devices, capacity * words, size),
                ((0, 0), (0, mask_rows - capacity * words), (0, 0)),
            ),
            jnp.pad(codes.reshape(devices, 1, capacity), ((0, 0), (0, 7), (0, size - capacity))),
        ],
        axis=1,
    )
    params = jnp.pad(jnp.stack([att_src, att_dst, out_bias]), ((0, 5), (0, -head_dims % 128)))
    chips = devices // 2
    across = 2 if chips % 2 == 0 else 1
    ways = (chips // across, across)
    chunks = math.gcd(blocks, max(1, 128 // devices))
    items = chunks + 1
    slots = devices * capacity
    whole = pl.BlockSpec(memory_space=VMEM)
    dma = pltpu.SemaphoreType.DMA
    tile_feats, tile_source, masks, codes, feats, source, target = pl.pallas_call(
        functools.partial(first_kernel, heads, capacity, chunks, ways, peers),
        out_shape=(
            jax.ShapeDtypeStruct((slots, head_dims, size), jnp.bfloat16),
            jax.ShapeDtypeStruct((slots, padded, size), jnp.float32),
            jax.ShapeDtypeStruct((devices, mask_rows, size), jnp.int32),
            jax.ShapeDtypeStruct((devices, 8, size), jnp.int32),
            jax.ShapeDtypeStruct((blocks, head_dims, size), jnp.bfloat16),
            jax.ShapeDtypeStruct((blocks, padded, size), jnp.float32),
            jax.ShapeDtypeStruct((blocks, padded, size), jnp.float32),
        ),
        in_specs=[whole] * 4,
        out_specs=(whole,) * 7,
        scratch_shapes=[
            VMEM((devices * blocks, head_dims, size), jnp.bfloat16),
            VMEM((devices * blocks, heads, size), jnp.float32),
            VMEM((chunks, peers * node_feats.shape[0], columns // chunks), jnp.bfloat16),
            VMEM((devices, mask_rows + 8, size), jnp.int32),
            pltpu.SMEM((devices, 8, size), jnp.int32),
            dma((4, devices, items)),
            dma((devices, items)),
            dma((max(1, peers - 1), chunks)),
            dma((max(1, peers - 1), chunks)),
            dma((devices - 1,)),
            dma((devices - 1,)),
            dma,
        ],
        compiler_params=pltpu.CompilerParams(
            collective_id=0, has_side_effects=True, vmem_limit_bytes=40 * 1024 * 1024
        ),
        name="gather",
    )(proj_weight, node_feats, params, payload)
    return pl.pallas_call(
        functools.partial(tile_kernel, heads, capacity),
        out_shape=jax.ShapeDtypeStruct((head_dims, columns), jnp.bfloat16),
        in_specs=[pl.BlockSpec(memory_space=pltpu.SMEM)] + [whole] * 8,
        out_specs=whole,
        scratch_shapes=[
            VMEM((blocks, head_dims, size), jnp.float32),
            VMEM((blocks, padded, size), jnp.float32),
            VMEM((blocks, padded, size), jnp.float32),
        ],
        compiler_params=pltpu.CompilerParams(vmem_limit_bytes=40 * 1024 * 1024),
        name="tiles",
    )(codes, masks, tile_feats, tile_source, feats, source, target, node_feats, params)


def solution(mesh):
    return jax.shard_map(
        local,
        mesh=mesh,
        in_specs=(
            P("mp", "dp"),
            P("mp", None),
            P("mp"),
            P("mp"),
            P("mp"),
            P("dp"),
            P("dp"),
            P("dp", None, None),
        ),
        out_specs=P("mp", "dp"),
        check_vma=False,
    )
```
